512 devices in a mesh: ckpt: 2 (over y), row: 32 (over z, core), col: 8 (over x).
Axes of the slice: x: 8, y: 2, z: 16, core: 2. Of those that a mesh axis runs over, the one named last changes fastest.
The devices are a block of a 8x16x16 slice.
Arguments:
- grad_slab: bfloat16 [768, 27648], P(('ckpt', 'col'), 'row'), parts along dimension 0, may hold values from -6 to 6
- eigenbasis: bfloat16 [55296, 14336], P(('ckpt', 'row'), 'col'), parts along dimension 0, may hold values from -0.0625 to 0.0625
- eigenvalues: bfloat16 [768, 14336], P('ckpt', 'col'), parts along dimension 0, may hold values from 0.049804688 to 5
Outputs:
- preconditioned: bfloat16 [768, 27648], P(('ckpt', 'col'), 'row'), parts along dimension 0
The draws below stay inside these ranges and needn't reach their ends.
There are 2 independent parts, one for each index of `ckpt`. The reference program is written for one: setup_inputs(seed, part) draws one part's arguments, and reference() takes and returns one part's arrays. A program takes and returns all parts, laid end to end along the dimension named above; each array names one. Nothing has to cross between parts.
All inputs are finite; a program needn't handle non-finite values.
Results may differ from the reference program's by a relative error of at most 0.0046.
Values may be sent and summed in bfloat16 or wider, within the bound.
A program may use at most 64 MiB of HBM per device.

```python
import math
import jax
import jax.numpy as jnp
from jax import lax

FF = 27648
EIGW = 14336
S = 384


def raised(entries, key, source, target, shards_of, factor):
    owner, partner = [(jnp.arange(entries.shape[dim]) // (entries.shape[dim] // shards_of)).reshape([-1 if axis == dim else 1 for axis in range(entries.ndim)]) for dim in (source, target)]
    chosen = jax.random.permutation(key, shards_of)[partner]
    strong = (owner == chosen) | (owner == (partner + shards_of // 2) % shards_of)
    return jnp.where(strong, factor * entries, entries)


def levels(stream_key, extent, shards, low, top_value):
    level = 1.0
    for dim, parts in shards:
        heights = jax.random.uniform(jax.random.fold_in(jax.random.fold_in(stream_key, 6), dim), (parts,), jnp.float32, low / len(shards), top_value / len(shards))
        level = level * jnp.repeat(jnp.exp(heights), extent[dim] // parts).reshape((-1,) + (1,) * (len(extent) - 1 - dim))
    return level


def noise(stream_key, shape, spread, limit, pieces=(), kind=jnp.bfloat16):
    level = levels(stream_key, shape, pieces, -0.22, 0.18) if pieces else 1.0
    values = jax.random.normal(stream_key, shape, jnp.float32) * spread * level
    return jnp.minimum(jnp.maximum(values, -limit), limit).astype(kind)


def bell_draw_with(stream_key, shape, scale, most, pieces, heavy, kind=jnp.bfloat16):
    values = scale * jax.random.normal(stream_key, shape, jnp.float32)
    if pieces:
        values = values * levels(stream_key, shape, pieces, -0.22, 0.18)
    return jnp.clip(raised(values, jax.random.fold_in(stream_key, 3), *heavy), -most, most).astype(kind)


def setup_inputs(seed: int = 0, part: int = 0) -> dict:
    splits = jax.random.split(jax.random.key(seed), 4)
    own_keys = jax.random.split(jax.random.fold_in(splits[3], part), 4)
    return {
        "grad_slab": noise(own_keys[0], (S, FF), 1.0, 6.0, ((0, 8), (1, 32))),
        "eigenbasis": bell_draw_with(own_keys[1], (FF, EIGW), FF ** -0.5, 0.0625, ((0, 32), (1, 8)), (0, 1, 32, 2.75)),
        "eigenvalues": jnp.clip(jnp.exp(math.log(5.0) - 4.609084 * jax.random.uniform(own_keys[2], (S, EIGW), jnp.float32) ** levels(own_keys[2], (S, EIGW), ((1, 8),), -0.2, 0.2)), 0.049804688, 5.0).astype(jnp.bfloat16),
    }


DAMPING = 0.1


def reference(grad_slab, eigenbasis, eigenvalues):
    rotated = jnp.dot(grad_slab, eigenbasis, preferred_element_type=jnp.float32)
    scaled = (rotated / (eigenvalues.astype(jnp.float32) + DAMPING)).astype(jnp.bfloat16)
    result = lax.dot_general(scaled, eigenbasis, (((1,), (1,)), ((), ())), preferred_element_type=jnp.float32)
    return result.astype(jnp.bfloat16)
```

```python
import functools

import jax
import jax.numpy as jnp
from jax import lax
from jax.experimental import pallas as pl
from jax.experimental.pallas import tpu as pltpu
from jax.sharding import PartitionSpec as P

DAMPING = 0.1
MESH = pl.DeviceIdType.MESH
CORES = 2
CHUNKS = 3
NZ = 16
NX = 8
BF16 = jnp.bfloat16
F32 = jnp.float32
N_SEMS = 48


class Labels:
    def __init__(self):
        self.index = {}

    def __call__(self, k, *label):
        return self.index.setdefault((k, *label), len(self.index))


def kernel(
    grad, eig, values, out,
    e_v, g_all, ev, psend, precv, acc,
    b1s, b1r, b2s, b2r, b3s, b3r, sc, res, d1s, d1r, d2s, d2r,
    local_sem, send_sem, recv_sem,
):
    r = lax.axis_index("row")
    x = lax.axis_index("col")
    z, c = lax.div(r, CORES), lax.rem(r, CORES)
    other = 1 - c
    unit_rows, half = acc.shape[2], acc.shape[3]
    h = g_all.shape[2]
    sem = Labels()
    started = []

    def copy(src, dst, index, row, col):
        return pltpu.make_async_remote_copy(
            src_ref=src, dst_ref=dst, send_sem=send_sem.at[index], recv_sem=recv_sem.at[index],
            device_id={"row": row, "col": col}, device_id_type=MESH,
        )

    def send(src, dst, index, row, col):
        c_ = copy(src, dst, index, row, col)
        c_.start()
        started.append(c_)

    def arrived(dst, index):
        copy(dst, dst, index, CORES * z + other, x).wait_recv()

    def zrow(offset):
        return lax.rem(z + (offset + NZ), NZ) * CORES + c

    def zunit(offset):
        return lax.rem(z + (offset + NZ), NZ)

    def xcol(offset):
        return lax.rem(x + (offset + NX), NX)

    loads = []
    own_g = []
    for k in range(CHUNKS):
        own_g.append(pltpu.make_async_copy(
            grad.at[pl.ds(k * h, h)], g_all.at[k, x], local_sem.at[1 + k]))
        own_g[-1].start()
    load_e = pltpu.make_async_copy(eig, e_v, local_sem.at[0])
    load_e.start()
    block = lax.div(z, 2)
    for k in range(CHUNKS):
        first = block * (CHUNKS * h) + k * h + lax.rem(z, 2) * unit_rows
        loads.append(pltpu.make_async_copy(
            values.at[pl.ds(pl.multiple_of(first, unit_rows), unit_rows),
                      pl.ds(pl.multiple_of(c * half, 128), half)],
            ev.at[k], local_sem.at[1 + CHUNKS + k]))
        loads[-1].start()

    barrier = pltpu.get_barrier_semaphore()
    partners = [(CORES * z + other, x)]
    partners += [(zrow(o), x) for o in (1, -1, 2, -2, 5, -5)]
    partners += [(r, xcol(o)) for o in (1, -1, 3, -3)]
    for row, col in partners:
        pl.semaphore_signal(barrier, inc=1, device_id={"row": row, "col": col}, device_id_type=MESH)
    pl.semaphore_wait(barrier, len(partners))

    def steps_of(k):
        s = -1 if k % 2 else 1
        zz_row = lambda o: zrow(s * o)
        zz = lambda o: zunit(s * o)
        xx = lambda o: xcol(s * o)
        own_cols = pl.ds(pl.multiple_of(c * half, 128), half)
        other_cols = pl.ds(pl.multiple_of(other * half, 128), half)
        peer = CORES * z + other

        def a_send(block_at, label, to):
            send(g_all.at[k, block_at], g_all.at[k, block_at], sem(k, *label), r, to)

        def a_wait(block_at, label):
            arrived(g_all.at[k, block_at], sem(k, *label))

        def a0():
            own_g[k].wait()
            a_send(x, ("ad", 1), xx(1))
            a_send(x, ("ae", 1), xx(-1))

        def a_round(n):
            def step():
                a_wait(xx(-n), ("ad", n))
                if n < 4:
                    a_send(xx(-n), ("ad", n + 1), xx(1))
                    a_wait(xx(n), ("ae", n))
                    if n < 3:
                        a_send(xx(n), ("ae", n + 1), xx(-1))
            return step

        def m1():
            if k == 0:
                load_e.wait()
            g = g_all[k].reshape(NX * h, g_all.shape[3])
            p = jnp.dot(g, e_v[:, other_cols], preferred_element_type=F32)
            psend[k] = p.astype(BF16).reshape(psend.shape[1:])
            send(psend.at[k], precv.at[k], sem(k, "x"), peer, x)
            p = jnp.dot(g, e_v[:, own_cols], preferred_element_type=F32)
            acc[k] = p.reshape(acc.shape[1:])
            arrived(precv.at[k], sem(k, "x"))
            acc[k] = acc[k] + precv[k].astype(F32)
            for slot, d in enumerate((4, 8, 2, 6)):
                b1s[k, slot] = acc[k, zz(-d)].astype(BF16)
            for slot, e in enumerate((4, 2, 6)):
                b1s[k, 4 + slot] = acc[k, zz(e)].astype(BF16)
            for name, lo, n, to in (("b1a", 0, 2, -1), ("b1b", 4, 1, 1), ("b1c", 2, 2, -1), ("b1d", 5, 2, 1)):
                send(b1s.at[k, pl.ds(lo, n)], b1r.at[k, pl.ds(lo, n)], sem(k, name), zz_row(to), x)

        def l2():
            arrived(b1r.at[k, pl.ds(0, 2)], sem(k, "b1a"))
            arrived(b1r.at[k, pl.ds(4, 1)], sem(k, "b1b"))
            for slot, d in enumerate((3, 7)):
                b2s[k, slot] = (acc[k, zz(-d)] + b1r[k, slot].astype(F32)).astype(BF16)
            b2s[k, 2] = (acc[k, zz(3)] + b1r[k, 4].astype(F32)).astype(BF16)
            b2s[k, 3] = acc[k, zz(7)].astype(BF16)
            for name, lo, to in (("b2a", 0, -2), ("b2b", 2, 2)):
                send(b2s.at[k, pl.ds(lo, 2)], b2r.at[k, pl.ds(lo, 2)], sem(k, name), zz_row(to), x)

        def l3():
            arrived(b1r.at[k, pl.ds(2, 2)], sem(k, "b1c"))
            arrived(b1r.at[k, pl.ds(5, 2)], sem(k, "b1d"))
            arrived(b2r.at[k, pl.ds(0, 2)], sem(k, "b2a"))
            arrived(b2r.at[k, pl.ds(2, 2)], sem(k, "b2b"))
            for slot, o, one, two in ((1, -5, 3, 1), (3, 5, 6, 3), (0, -1, 2, 0), (2, 1, 5, 2)):
                b3s[k, slot] = (
                    acc[k, zz(o)] + b1r[k, one].astype(F32) + b2r[k, two].astype(F32)
                ).astype(BF16)
                send(b3s.at[k, slot], b3r.at[k, slot], sem(k, "b3", slot), zz_row(o), x)

        def to_peer(unit):
            send_ = copy(sc.at[c, k, unit], sc.at[c, k, unit], sem(k, "p"), peer, x)
            send_.start()

        def c_send(unit, label, o):
            send(sc.at[c, k, unit], sc.at[c, k, unit], sem(k, *label), zz_row(o), x)

        def c_wait(unit, label):
            arrived(sc.at[c, k, unit], sem(k, *label))

        def final():
            for slot in range(4):
                arrived(b3r.at[k, slot], sem(k, "b3", slot))
            loads[k].wait()
            total = acc[k, z]
            for slot in range(4):
                total = total + b3r[k, slot].astype(F32)
            sc[c, k, z] = (total / (ev[k].astype(F32) + DAMPING)).astype(BF16)
            c_send(z, ("cd", 5), 5)
            c_send(z, ("ce", 5), -5)
            c_send(z, ("cd", 1), 1)
            c_send(z, ("ce", 1), -1)
            to_peer(z)

        def c1():
            for way, t in (("cd", 1), ("ce", -1)):
                for n in (1, 5):
                    c_wait(zz(-t * n), (way, n))
                    c_send(zz(-t * n), (way, n + 2), 2 * t)
            for way, t in (("cd", 1), ("ce", -1)):
                for n in (1, 5):
                    c_send(zz(-t * n), (way, n + 1), t)
                    to_peer(zz(-t * n))

        def c2():
            for way, t in (("cd", 1), ("ce", -1)):
                for n in (3, 7):
                    c_wait(zz(-t * n), (way, n))
                    if (way, n) != ("ce", 7):
                        c_send(zz(-t * n), (way, n + 1), t)
            for t in (1, -1):
                for n in (3, 7):
                    to_peer(zz(-t * n))

        def c3():
            for way, t in (("cd", 1), ("ce", -1)):
                for n in (2, 6, 4, 8):
                    if (way, n) != ("ce", 8):
                        c_wait(zz(-t * n), (way, n))
                        to_peer(zz(-t * n))

        def by_columns(lhs, cols):
            return lax.dot_general(
                lhs, e_v[:, cols], (((1,), (1,)), ((), ())), preferred_element_type=F32)

        def m2():
            p = by_columns(sc[c, k].reshape(NZ * unit_rows, half), own_cols)
            copy(sc.at[other, k], sc.at[other, k], sem(k, "p"), peer, x).wait_recv()
            p = p + by_columns(sc[other, k].reshape(NZ * unit_rows, half), other_cols)
            res[k] = p.reshape(res.shape[1:])
            for slot, o in enumerate((-2, -4, 2)):
                d1s[k, slot] = res[k, xx(o)].astype(BF16)
                to = -1 if o < 0 else 1
                send(d1s.at[k, slot], d1r.at[k, slot], sem(k, "d1", slot), r, xx(to))

        def d2():
            for slot, o, one in ((1, -3, 1), (3, 3, None), (0, -1, 0), (2, 1, 2)):
                value = res[k, xx(o)]
                if one is not None:
                    arrived(d1r.at[k, one], sem(k, "d1", one))
                    value = value + d1r[k, one].astype(F32)
                d2s[k, slot] = value.astype(BF16)
                send(d2s.at[k, slot], d2r.at[k, slot], sem(k, "d2", slot), r, xx(o))

        def df():
            total = res[k, x]
            for slot in range(4):
                arrived(d2r.at[k, slot], sem(k, "d2", slot))
                total = total + d2r[k, slot].astype(F32)
            out[pl.ds(k * h, h)] = total.astype(BF16)

        return [a0, a_round(1), a_round(2), a_round(3), a_round(4), m1, l2, l3, final, c1, c2, c3, m2, d2, df]

    chunks = [steps_of(k) for k in range(CHUNKS)]
    for k in range(CHUNKS):
        chunks[k][0]()
    length = len(chunks[0]) - 1
    for t in range(length + CHUNKS - 1):
        for k in range(CHUNKS):
            if 0 <= t - k < length:
                chunks[k][1 + t - k]()

    for c_ in started:
        c_.wait_send()
    for k in range(CHUNKS):
        copy(sc.at[c, k], sc.at[c, k], sem(k, "p"), CORES * z + other, x).wait_send()


def on_device(grad_slab, eigenbasis, eigenvalues):
    rows, depth = grad_slab.shape
    width = eigenbasis.shape[1]
    half = width // CORES
    h = rows // CHUNKS
    unit_rows = h * NX // NZ
    unit = (unit_rows, half)
    own = (h, depth)
    any_ = pl.BlockSpec(memory_space=pl.ANY)
    vmem = lambda lead, last, kind=BF16: pltpu.VMEM((CHUNKS, *lead, *last), kind)
    return pl.pallas_call(
        kernel,
        out_shape=jax.ShapeDtypeStruct((rows, depth), BF16),
        in_specs=[any_] * 3,
        out_specs=pl.BlockSpec(memory_space=pltpu.VMEM),
        scratch_shapes=[
            pltpu.VMEM(eigenbasis.shape, BF16),
            vmem((NX,), own),
            vmem((), unit),
            vmem((NZ,), unit),
            vmem((NZ,), unit),
            vmem((NZ,), unit, F32),
            vmem((7,), unit),
            vmem((7,), unit),
            vmem((4,), unit),
            vmem((4,), unit),
            vmem((4,), unit),
            vmem((4,), unit),
            pltpu.VMEM((CORES, CHUNKS, NZ, *unit), BF16),
            vmem((NX,), own, F32),
            vmem((3,), own),
            vmem((3,), own),
            vmem((4,), own),
            vmem((4,), own),
            pltpu.SemaphoreType.DMA((1 + 2 * CHUNKS,)),
            pltpu.SemaphoreType.DMA((N_SEMS * CHUNKS,)),
            pltpu.SemaphoreType.DMA((N_SEMS * CHUNKS,)),
        ],
        compiler_params=pltpu.CompilerParams(
            collective_id=0, has_side_effects=True, vmem_limit_bytes=48 * 1024 * 1024
        ),
    )(grad_slab, eigenbasis, eigenvalues)


def solution(mesh):
    return jax.shard_map(
        on_device,
        mesh=mesh,
        in_specs=(P(("ckpt", "col"), "row"), P(("ckpt", "row"), "col"), P("ckpt", "col")),
        out_specs=P(("ckpt", "col"), "row"),
        check_vma=False,
    )
```

```python
import functools

import jax
import jax.numpy as jnp
from jax import lax
from jax.experimental import pallas as pl
from jax.experimental.pallas import tpu as pltpu
from jax.sharding import PartitionSpec as P

DAMPING = 0.1
MESH = pl.DeviceIdType.MESH
CORES = 2
CHUNKS = 3
NZ = 16
NX = 8
BF16 = jnp.bfloat16
F32 = jnp.float32
N_SEMS = 48
GAP = 3.3
LEVEL_ONE = (
    ("fa", 1, (-5, 7)), ("fb", -1, (-7, 5)), ("fc", -2, (-8,)),
    ("na", 1, (-1, 3)), ("nb", -1, (-3, 1)), ("nc", -2, (-4,)), ("nd", 2, (4,)),
)


class Labels:
    def __init__(self):
        self.index = {}

    def __call__(self, k, *label):
        return self.index.setdefault((k, *label), len(self.index))


def kernel(
    grad, eig, values, out,
    e_v, g_all, ev, psend, precv, acc,
    b1s, b1r, b2s, b2r, sc, res, d1s, d1r, d2s, d2r,
    local_sem, send_sem, recv_sem,
):
    r = lax.axis_index("row")
    x = lax.axis_index("col")
    z, c = lax.div(r, CORES), lax.rem(r, CORES)
    other = 1 - c
    unit_rows, half = acc.shape[2], acc.shape[3]
    h = g_all.shape[2]
    sem = Labels()
    started = []

    def copy(src, dst, index, row, col):
        return pltpu.make_async_remote_copy(
            src_ref=src, dst_ref=dst, send_sem=send_sem.at[index], recv_sem=recv_sem.at[index],
            device_id={"row": row, "col": col}, device_id_type=MESH,
        )

    def send(src, dst, index, row, col):
        c_ = copy(src, dst, index, row, col)
        c_.start()
        started.append(c_)

    def arrived(dst, index):
        copy(dst, dst, index, CORES * z + other, x).wait_recv()

    def zrow(offset):
        return lax.rem(z + (offset + NZ), NZ) * CORES + c

    def zunit(offset):
        return lax.rem(z + (offset + NZ), NZ)

    def xcol(offset):
        return lax.rem(x + (offset + NX), NX)

    loads = []
    own_g = []
    for k in range(CHUNKS):
        own_g.append(pltpu.make_async_copy(
            grad.at[pl.ds(k * h, h)], g_all.at[k, x], local_sem.at[1 + k]))
        own_g[-1].start()
    load_e = pltpu.make_async_copy(eig, e_v, local_sem.at[0])
    load_e.start()
    block = lax.div(z, 2)
    for k in range(CHUNKS):
        first = block * (CHUNKS * h) + k * h + lax.rem(z, 2) * unit_rows
        loads.append(pltpu.make_async_copy(
            values.at[pl.ds(pl.multiple_of(first, unit_rows), unit_rows),
                      pl.ds(pl.multiple_of(c * half, 128), half)],
            ev.at[k], local_sem.at[1 + CHUNKS + k]))
        loads[-1].start()

    barrier = pltpu.get_barrier_semaphore()
    partners = [(CORES * z + other, x)]
    partners += [(zrow(o), x) for o in (1, -1, 2, -2, 6, -6)]
    partners += [(r, xcol(o)) for o in (1, -1, 3, -3)]
    for row, col in partners:
        pl.semaphore_signal(barrier, inc=1, device_id={"row": row, "col": col}, device_id_type=MESH)
    pl.semaphore_wait(barrier, len(partners))

    def steps_of(k):
        s = -1 if k % 2 else 1
        zz_row = lambda o: zrow(s * o)
        zz = lambda o: zunit(s * o)
        xx = lambda o: xcol(s * o)
        own_cols = pl.ds(pl.multiple_of(c * half, 128), half)
        other_cols = pl.ds(pl.multiple_of(other * half, 128), half)
        peer = CORES * z + other

        def a_send(block_at, label, to):
            send(g_all.at[k, block_at], g_all.at[k, block_at], sem(k, *label), r, to)

        def a_wait(block_at, label):
            arrived(g_all.at[k, block_at], sem(k, *label))

        def a0():
            own_g[k].wait()
            for way, t in (("ad", 1), ("ae", -1)):
                for n in (3, 1):
                    a_send(x, (way, n), xx(t * n))

        def a_near():
            for way, t in (("ad", 1), ("ae", -1)):
                a_wait(xx(-t), (way, 1))
                a_send(xx(-t), (way, 2), xx(t))

        def a_far():
            a_wait(xx(-3), ("ad", 3))
            a_send(xx(-3), ("ad", 4), xx(1))
            a_wait(xx(3), ("ae", 3))

        def m1():
            a_wait(xx(-2), ("ad", 2))
            a_wait(xx(2), ("ae", 2))
            a_wait(xx(-4), ("ad", 4))
            if k == 0:
                load_e.wait()
            g = g_all[k].reshape(NX * h, g_all.shape[3])
            p = jnp.dot(g, e_v[:, other_cols], preferred_element_type=F32)
            psend[k] = p.astype(BF16).reshape(psend.shape[1:])
            send(psend.at[k], precv.at[k], sem(k, "x"), peer, x)
            p = jnp.dot(g, e_v[:, own_cols], preferred_element_type=F32)
            acc[k] = p.reshape(acc.shape[1:])

        def m1_sum():
            arrived(precv.at[k], sem(k, "x"))
            acc[k] = acc[k] + precv[k].astype(F32)
            slot = 0
            for name, to, units in LEVEL_ONE:
                for o in units:
                    b1s[k, slot] = acc[k, zz(o)].astype(BF16)
                    slot += 1
                n = len(units)
                part = pl.ds(slot - n, n)
                send(b1s.at[k, part], b1r.at[k, part], sem(k, name), zz_row(to), x)

        def meet(names, sums):
            slot = 0
            for name, to, units in LEVEL_ONE:
                if name in names:
                    arrived(b1r.at[k, pl.ds(slot, len(units))], sem(k, name))
                slot += len(units)
            for slot, o, ones in sums:
                value = acc[k, zz(o)]
                for one in ones:
                    value = value + b1r[k, one].astype(F32)
                b2s[k, slot] = value.astype(BF16)
                send(b2s.at[k, slot], b2r.at[k, slot], sem(k, "b2", slot), zz_row(o), x)

        def meet_far():
            meet(("fa", "fb", "fc"), ((1, -6, (0, 2, 4)), (3, 6, (3, 1))))

        def meet_near():
            meet(("na", "nb", "nc", "nd"), ((0, -2, (5, 7, 9)), (2, 2, (8, 6, 10))))

        def to_peer(unit):
            send_ = copy(sc.at[c, k, unit], sc.at[c, k, unit], sem(k, "p"), peer, x)
            send_.start()

        def c_send(unit, label, o):
            send(sc.at[c, k, unit], sc.at[c, k, unit], sem(k, *label), zz_row(o), x)

        def c_wait(unit, label):
            arrived(sc.at[c, k, unit], sem(k, *label))

        def final():
            for slot in range(4):
                arrived(b2r.at[k, slot], sem(k, "b2", slot))
            loads[k].wait()
            total = acc[k, z]
            for slot in range(4):
                total = total + b2r[k, slot].astype(F32)
            sc[c, k, z] = (total / (ev[k].astype(F32) + DAMPING)).astype(BF16)
            for n in (6, 2):
                for way, t in (("cd", 1), ("ce", -1)):
                    c_send(z, (way, n), t * n)
            to_peer(z)

        def fan(n):
            for way, t in (("cd", 1), ("ce", -1)):
                unit = zz(-t * n)
                c_wait(unit, (way, n))
                for m in (2, -1, 1):
                    if (way, n + m) != ("ce", 8):
                        c_send(unit, (way, n + m), t * m)
            for t in (1, -1):
                to_peer(zz(-t * n))

        def c_near():
            fan(2)

        def c_far():
            fan(6)

        def c_end():
            for n in (1, 3, 4, 5, 7, 8):
                for way, t in (("cd", 1), ("ce", -1)):
                    if (way, n) != ("ce", 8):
                        c_wait(zz(-t * n), (way, n))
                        to_peer(zz(-t * n))

        def by_columns(lhs, cols):
            return lax.dot_general(
                lhs, e_v[:, cols], (((1,), (1,)), ((), ())), preferred_element_type=F32)

        def m2():
            p = by_columns(sc[c, k].reshape(NZ * unit_rows, half), own_cols)
            copy(sc.at[other, k], sc.at[other, k], sem(k, "p"), peer, x).wait_recv()
            p = p + by_columns(sc[other, k].reshape(NZ * unit_rows, half), other_cols)
            res[k] = p.reshape(res.shape[1:])
            for slot, o in enumerate((-2, -4, 2)):
                d1s[k, slot] = res[k, xx(o)].astype(BF16)
                to = -1 if o < 0 else 1
                send(d1s.at[k, slot], d1r.at[k, slot], sem(k, "d1", slot), r, xx(to))

        def d2():
            for slot, o, one in ((1, -3, 1), (3, 3, None), (0, -1, 0), (2, 1, 2)):
                value = res[k, xx(o)]
                if one is not None:
                    arrived(d1r.at[k, one], sem(k, "d1", one))
                    value = value + d1r[k, one].astype(F32)
                d2s[k, slot] = value.astype(BF16)
                send(d2s.at[k, slot], d2r.at[k, slot], sem(k, "d2", slot), r, xx(o))

        def df():
            total = res[k, x]
            for slot in range(4):
                arrived(d2r.at[k, slot], sem(k, "d2", slot))
                total = total + d2r[k, slot].astype(F32)
            out[pl.ds(k * h, h)] = total.astype(BF16)

        return [
            (0.0, a0), (3.4, a_near), (6.0, a_far), (9.5, m1), (11.5, m1_sum),
            (16.5, meet_far), (17.0, meet_near), (25.0, final),
            (29.5, c_near), (33.0, c_far), (37.0, c_end), (37.1, m2), (42.0, d2), (48.0, df),
        ]

    plan = []
    for k in range(CHUNKS):
        plan += [(at + GAP * k, k, step) for at, step in steps_of(k)]
    for _, _, step in sorted(plan, key=lambda item: item[:2]):
        step()

    for c_ in started:
        c_.wait_send()
    for k in range(CHUNKS):
        copy(sc.at[c, k], sc.at[c, k], sem(k, "p"), CORES * z + other, x).wait_send()


def on_device(grad_slab, eigenbasis, eigenvalues):
    rows, depth = grad_slab.shape
    width = eigenbasis.shape[1]
    half = width // CORES
    h = rows // CHUNKS
    unit_rows = h * NX // NZ
    unit = (unit_rows, half)
    own = (h, depth)
    any_ = pl.BlockSpec(memory_space=pltpu.HBM)
    vmem = lambda lead, last, kind=BF16: pltpu.VMEM((CHUNKS, *lead, *last), kind)
    return pl.pallas_call(
        kernel,
        out_shape=jax.ShapeDtypeStruct((rows, depth), BF16),
        in_specs=[any_] * 3,
        out_specs=pl.BlockSpec(memory_space=pltpu.VMEM),
        scratch_shapes=[
            pltpu.VMEM(eigenbasis.shape, BF16),
            vmem((NX,), own),
            vmem((), unit),
            vmem((NZ,), unit),
            vmem((NZ,), unit),
            vmem((NZ,), unit, F32),
            vmem((11,), unit),
            vmem((11,), unit),
            vmem((4,), unit),
            vmem((4,), unit),
            pltpu.VMEM((CORES, CHUNKS, NZ, *unit), BF16),
            vmem((NX,), own, F32),
            vmem((3,), own),
            vmem((3,), own),
            vmem((4,), own),
            vmem((4,), own),
            pltpu.SemaphoreType.DMA((1 + 2 * CHUNKS,)),
            pltpu.SemaphoreType.DMA((N_SEMS * CHUNKS,)),
            pltpu.SemaphoreType.DMA((N_SEMS * CHUNKS,)),
        ],
        compiler_params=pltpu.CompilerParams(
            collective_id=0, has_side_effects=True, vmem_limit_bytes=67043328
        ),
    )(grad_slab, eigenbasis, eigenvalues)


def solution(mesh):
    return jax.shard_map(
        on_device,
        mesh=mesh,
        in_specs=(P(("ckpt", "col"), "row"), P(("ckpt", "row"), "col"), P("ckpt", "col")),
        out_specs=P(("ckpt", "col"), "row"),
        check_vma=False,
    )
```

```python
import functools

import jax
import jax.numpy as jnp
from jax import lax
from jax.experimental import pallas as pl
from jax.experimental.pallas import tpu as pltpu
from jax.sharding import PartitionSpec as P

DAMPING = 0.1
MESH = pl.DeviceIdType.MESH
CORES = 2
CHUNKS = 3
NZ = 16
NX = 8
BF16 = jnp.bfloat16
F32 = jnp.float32
SENT = ("g", "x", "b1", "b2", "b3", "c", "p", "d1", "d2")
ARRIVE = ("a2", "a", "x", "far", "near", "b2", "b3", "c3", "c6", "c", "p", "d1", "d2")
GAP = 3.7
LEVEL_ONE = (
    ("far", 1, (-5, 7)), ("far", -1, (-7, 5)), ("far", -2, (-8,)),
    ("near", 1, (-2, 4)), ("near", -1, (-4, 2)),
)


def kernel(
    grad, eig, values, out,
    e_v, g_all, ev, psend, precv, acc,
    b1s, b1r, b2s, b2r, b3s, b3r, sc, res, d1s, d1r, d2s, d2r,
    local_sem, send_sem, recv_sem,
):
    r = lax.axis_index("row")
    x = lax.axis_index("col")
    z, c = lax.div(r, CORES), lax.rem(r, CORES)
    other = 1 - c
    unit_rows, half = acc.shape[2], acc.shape[3]
    h = g_all.shape[2]

    def send(k, src, dst, sent, arrive, row, col):
        pltpu.make_async_remote_copy(
            src_ref=src, dst_ref=dst, send_sem=send_sem.at[SENT.index(sent)],
            recv_sem=recv_sem.at[k * len(ARRIVE) + ARRIVE.index(arrive)],
            device_id={"row": row, "col": col}, device_id_type=MESH,
        ).start()

    def pending(ref, sent=0, arrive=0):
        return pltpu.make_async_remote_copy(
            src_ref=ref, dst_ref=ref, send_sem=send_sem.at[sent], recv_sem=recv_sem.at[arrive],
            device_id={"row": CORES * z + other, "col": x}, device_id_type=MESH,
        )

    def arrived(k, ref, arrive):
        pending(ref, arrive=k * len(ARRIVE) + ARRIVE.index(arrive)).wait_recv()

    def all_sent(ref, sent):
        pending(ref, sent=SENT.index(sent)).wait_send()

    def zrow(offset):
        return lax.rem(z + (offset + NZ), NZ) * CORES + c

    def zunit(offset):
        return lax.rem(z + (offset + NZ), NZ)

    def xcol(offset):
        return lax.rem(x + (offset + NX), NX)

    for k in range(CHUNKS):
        pltpu.make_async_copy(grad.at[pl.ds(k * h, h)], g_all.at[k, x], local_sem.at[0]).start()
    pltpu.make_async_copy(eig, e_v, local_sem.at[1]).start()
    block = lax.div(z, 2)
    for k in range(CHUNKS):
        first = block * (CHUNKS * h) + k * h + lax.rem(z, 2) * unit_rows
        pltpu.make_async_copy(
            values.at[pl.ds(pl.multiple_of(first, unit_rows), unit_rows),
                      pl.ds(pl.multiple_of(c * half, 128), half)],
            ev.at[k], local_sem.at[2]).start()

    def loaded(ref, index):
        pltpu.make_async_copy(ref, ref, local_sem.at[index]).wait()

    barrier = pltpu.get_barrier_semaphore()
    partners = [(CORES * z + other, x)]
    partners += [(zrow(o), x) for o in (1, -1, 2, -2, 3, -3)]
    partners += [(r, xcol(o)) for o in (1, -1, 2, -2)]
    for row, col in partners:
        pl.semaphore_signal(barrier, inc=1, device_id={"row": row, "col": col}, device_id_type=MESH)
    pl.semaphore_wait(barrier, len(partners))

    def steps_of(k):
        s = -1 if k % 2 else 1
        zz_row = lambda o: zrow(s * o)
        zz = lambda o: zunit(s * o)
        xx = lambda o: xcol(s * o)
        own_cols = pl.ds(pl.multiple_of(c * half, 128), half)
        other_cols = pl.ds(pl.multiple_of(other * half, 128), half)
        peer = CORES * z + other

        def a_send(o, n, to):
            block_at = g_all.at[k, xx(o)]
            send(k, block_at, block_at, "g", "a2" if n == 2 else "a", r, xx(to))

        def a0():
            if k == 0:
                loaded(g_all.at[:, x], 0)
            for n in (2, 1):
                a_send(0, n, n)
                a_send(0, n, -n)

        def a_pass():
            arrived(k, g_all.at[k, pl.ds(0, 2)], "a2")
            a_send(-2, 4, 2)
            a_send(-2, 3, 1)
            a_send(2, 3, -1)

        def m1():
            arrived(k, g_all.at[k, pl.ds(0, 5)], "a")
            if k == 0:
                loaded(e_v, 1)
            g = g_all[k].reshape(NX * h, g_all.shape[3])
            p = jnp.dot(g, e_v[:, other_cols], preferred_element_type=F32)
            psend[k] = p.astype(BF16).reshape(psend.shape[1:])
            send(k, psend.at[k], precv.at[k], "x", "x", peer, x)
            p = jnp.dot(g, e_v[:, own_cols], preferred_element_type=F32)
            acc[k] = p.reshape(acc.shape[1:])

        def m1_sum():
            arrived(k, precv.at[k], "x")
            acc[k] = acc[k] + precv[k].astype(F32)
            slot = 0
            for arrive, to, units in LEVEL_ONE:
                for o in units:
                    b1s[k, slot] = acc[k, zz(o)].astype(BF16)
                    slot += 1
                n = len(units)
                part = pl.ds(slot - n, n)
                send(k, b1s.at[k, part], b1r.at[k, part], "b1", arrive, zz_row(to), x)
            for slot, o in ((2, -1), (3, 1)):
                b3s[k, slot] = acc[k, zz(o)].astype(BF16)
                send(k, b3s.at[k, slot], b3r.at[k, slot], "b3", "b3", zz_row(o), x)

        def level_one_sum(o, slots):
            value = acc[k, zz(o)]
            for slot in slots:
                value = value + b1r[k, slot].astype(F32)
            return value

        def meet_far():
            arrived(k, b1r.at[k, pl.ds(0, 5)], "far")
            for slot, o, slots, to in ((0, -6, (0, 2, 4), -3), (1, 6, (3, 1), 3)):
                b2s[k, slot] = level_one_sum(o, slots).astype(BF16)
                send(k, b2s.at[k, slot], b2r.at[k, slot], "b2", "b2", zz_row(to), x)

        def meet_near():
            arrived(k, b1r.at[k, pl.ds(5, 4)], "near")
            arrived(k, b2r.at[k], "b2")
            for slot, o, slots in ((0, -3, (5, 7)), (1, 3, (8, 6))):
                value = level_one_sum(o, slots) + b2r[k, slot].astype(F32)
                b3s[k, slot] = value.astype(BF16)
                send(k, b3s.at[k, slot], b3r.at[k, slot], "b3", "b3", zz_row(o), x)

        def to_peer(unit):
            at = sc.at[c, k, unit]
            send(k, at, at, "p", "p", peer, x)

        def c_send(unit, n, o):
            at = sc.at[c, k, unit]
            send(k, at, at, "c", "c%d" % n if n in (3, 6) else "c", zz_row(o), x)

        def final():
            arrived(k, b3r.at[k], "b3")
            if k == 0:
                loaded(ev, 2)
            total = acc[k, z]
            for slot in range(4):
                total = total + b3r[k, slot].astype(F32)
            sc[c, k, z] = (total / (ev[k].astype(F32) + DAMPING)).astype(BF16)
            for n in (3, 1):
                c_send(z, n, n)
                c_send(z, n, -n)
            to_peer(z)

        def fan(n, moves):
            arrived(k, sc.at[c, k, pl.ds(0, 2)], "c%d" % n)
            for t in (1, -1):
                for m in moves:
                    if t * (n + m) != -8:
                        c_send(zz(-t * n), n + m, t * m)
            for t in (1, -1):
                to_peer(zz(-t * n))

        def c_near():
            fan(3, (3, -1, 1))

        def c_far():
            fan(6, (2, -1, 1))

        def c_end():
            arrived(k, sc.at[c, k, pl.ds(0, 11)], "c")
            for n in (1, 2, 4, 5, 7, 8):
                for t in (1, -1):
                    if t * n != -8:
                        to_peer(zz(-t * n))

        def by_columns(lhs, cols):
            return lax.dot_general(
                lhs, e_v[:, cols], (((1,), (1,)), ((), ())), preferred_element_type=F32)

        def m2():
            p = by_columns(sc[c, k].reshape(NZ * unit_rows, half), own_cols)
            arrived(k, sc.at[other, k], "p")
            p = p + by_columns(sc[other, k].reshape(NZ * unit_rows, half), other_cols)
            res[k] = p.reshape(res.shape[1:])
            for slot, o, to in ((0, -4, -2), (1, -3, -1), (2, 3, 1)):
                d1s[k, slot] = res[k, xx(o)].astype(BF16)
                send(k, d1s.at[k, slot], d1r.at[k, slot], "d1", "d1", r, xx(to))
            for slot, o in ((2, -1), (3, 1)):
                d2s[k, slot] = res[k, xx(o)].astype(BF16)
                send(k, d2s.at[k, slot], d2r.at[k, slot], "d2", "d2", r, xx(o))

        def d2():
            arrived(k, d1r.at[k], "d1")
            for slot, o, ones in ((0, -2, (0, 1)), (1, 2, (2,))):
                value = res[k, xx(o)]
                for one in ones:
                    value = value + d1r[k, one].astype(F32)
                d2s[k, slot] = value.astype(BF16)
                send(k, d2s.at[k, slot], d2r.at[k, slot], "d2", "d2", r, xx(o))

        def df():
            arrived(k, d2r.at[k], "d2")
            total = res[k, x]
            for slot in range(4):
                total = total + d2r[k, slot].astype(F32)
            out[pl.ds(k * h, h)] = total.astype(BF16)

        return [
            (0.0, a0), (5.0, a_pass), (9.0, m1), (11.5, m1_sum),
            (16.0, meet_far), (21.0, meet_near), (26.0, final),
            (31.0, c_near), (36.0, c_far), (40.5, c_end), (40.6, m2), (46.0, d2), (51.0, df),
        ]

    plan = []
    for k in range(CHUNKS):
        plan += [(at + GAP * k, k, step) for at, step in steps_of(k)]
    for _, _, step in sorted(plan, key=lambda item: item[:2]):
        step()

    for ref, sent in (
        (g_all.at[:, pl.ds(0, NX - 1)], "g"), (psend, "x"), (b1s, "b1"), (b2s, "b2"), (b3s, "b3"),
        (sc.at[c, :, pl.ds(0, NZ - 1)], "c"), (sc.at[c], "p"), (d1s, "d1"), (d2s, "d2"),
    ):
        all_sent(ref, sent)


def on_device(grad_slab, eigenbasis, eigenvalues):
    rows, depth = grad_slab.shape
    width = eigenbasis.shape[1]
    half = width // CORES
    h = rows // CHUNKS
    unit_rows = h * NX // NZ
    unit = (unit_rows, half)
    own = (h, depth)
    any_ = pl.BlockSpec(memory_space=pltpu.HBM)
    vmem = lambda lead, last, kind=BF16: pltpu.VMEM((CHUNKS, *lead, *last), kind)
    return pl.pallas_call(
        kernel,
        out_shape=jax.ShapeDtypeStruct((rows, depth), BF16),
        in_specs=[any_] * 3,
        out_specs=pl.BlockSpec(memory_space=pltpu.VMEM),
        scratch_shapes=[
            pltpu.VMEM(eigenbasis.shape, BF16),
            vmem((NX,), own),
            vmem((), unit),
            vmem((NZ,), unit),
            vmem((NZ,), unit),
            vmem((NZ,), unit, F32),
            vmem((9,), unit),
            vmem((9,), unit),
            vmem((2,), unit),
            vmem((2,), unit),
            vmem((4,), unit),
            vmem((4,), unit),
            pltpu.VMEM((CORES, CHUNKS, NZ, *unit), BF16),
            vmem((NX,), own, F32),
            vmem((3,), own),
            vmem((3,), own),
            vmem((4,), own),
            vmem((4,), own),
            pltpu.SemaphoreType.DMA((3,)),
            pltpu.SemaphoreType.DMA((len(SENT),)),
            pltpu.SemaphoreType.DMA((CHUNKS * len(ARRIVE),)),
        ],
        compiler_params=pltpu.CompilerParams(
            collective_id=0, has_side_effects=True, vmem_limit_bytes=67043328
        ),
    )(grad_slab, eigenbasis, eigenvalues)


def solution(mesh):
    return jax.shard_map(
        on_device,
        mesh=mesh,
        in_specs=(P(("ckpt", "col"), "row"), P(("ckpt", "row"), "col"), P("ckpt", "col")),
        out_specs=P(("ckpt", "col"), "row"),
        check_vma=False,
    )
```

```python
import functools

import jax
import jax.numpy as jnp
from jax import lax
from jax.experimental import pallas as pl
from jax.experimental.pallas import tpu as pltpu
from jax.sharding import PartitionSpec as P

DAMPING = 0.1
MESH = pl.DeviceIdType.MESH
CORES = 2
CHUNKS = 3
NZ = 16
NX = 8
BF16 = jnp.bfloat16
F32 = jnp.float32
SENT = ("g", "x", "b1", "b3", "c", "p", "d1", "d2")
ARRIVE = ("a2", "a", "x", "far", "near", "b3", "c2", "c5", "c", "p", "d1", "d2")
LEVEL_ONE = (
    ("far", -3, (-8,)), ("far", 1, (-4, 6)), ("far", -1, (-6, 4)), ("far", -2, (-7,)), ("far", 2, (7,)),
    ("near", 1, (-1, 3)), ("near", -1, (-3, 1)),
)
ORDER = (
    (0, "a0"), (1, "a0"), (None, "hello_1"), (0, "a_pass"), (None, "hello_2"),
    (2, "a0"), (1, "a_pass"), (0, "m1"), (0, "m1_sum"), (2, "a_pass"),
    (1, "m1"), (1, "m1_sum"), (2, "m1"), (None, "hello_3"), (0, "meet_far"),
    (2, "m1_sum"), (1, "meet_far"), (0, "meet_near"), (1, "meet_near"), (2, "meet_far"),
    (2, "meet_near"), (0, "final"), (1, "final"), (2, "final"), (0, "c_near"),
    (0, "c_far"), (1, "c_near"), (1, "c_far"), (2, "c_near"), (2, "c_far"),
    (0, "c_end"), (0, "m2"), (1, "c_end"), (2, "c_end"), (1, "m2"),
    (2, "m2"), (0, "d2"), (1, "d2"), (2, "d2"), (0, "df"),
    (1, "df"), (2, "df"),
)


def kernel(
    grad, eig, values, out,
    e_v, g_all, ev, psend, precv, acc,
    b1s, b1r, b3s, b3r, sc, res, d1s, d1r, d2s, d2r,
    local_sem, send_sem, recv_sem, word_sem,
):
    r = lax.axis_index("row")
    x = lax.axis_index("col")
    z, c = lax.div(r, CORES), lax.rem(r, CORES)
    other = 1 - c
    unit_rows, half = acc.shape[2], acc.shape[3]
    h = g_all.shape[2]

    def send(k, src, dst, sent, arrive, row, col):
        pltpu.make_async_remote_copy(
            src_ref=src, dst_ref=dst, send_sem=send_sem.at[SENT.index(sent)],
            recv_sem=recv_sem.at[k * len(ARRIVE) + ARRIVE.index(arrive)],
            device_id={"row": row, "col": col}, device_id_type=MESH,
        ).start()

    def pending(ref, sent=0, arrive=0):
        return pltpu.make_async_remote_copy(
            src_ref=ref, dst_ref=ref, send_sem=send_sem.at[sent], recv_sem=recv_sem.at[arrive],
            device_id={"row": CORES * z + other, "col": x}, device_id_type=MESH,
        )

    def arrived(k, ref, arrive):
        pending(ref, arrive=k * len(ARRIVE) + ARRIVE.index(arrive)).wait_recv()

    def all_sent(ref, sent):
        pending(ref, sent=SENT.index(sent)).wait_send()

    def zrow(offset):
        return lax.rem(z + (offset + NZ), NZ) * CORES + c

    def zunit(offset):
        return lax.rem(z + (offset + NZ), NZ)

    def xcol(offset):
        return lax.rem(x + (offset + NX), NX)

    for k in range(CHUNKS):
        pltpu.make_async_copy(grad.at[pl.ds(k * h, h)], g_all.at[k, x], local_sem.at[0]).start()
    pltpu.make_async_copy(eig, e_v, local_sem.at[1]).start()
    block = lax.div(z, 2)
    for k in range(CHUNKS):
        first = block * (CHUNKS * h) + k * h + lax.rem(z, 2) * unit_rows
        pltpu.make_async_copy(
            values.at[pl.ds(pl.multiple_of(first, unit_rows), unit_rows),
                      pl.ds(pl.multiple_of(c * half, 128), half)],
            ev.at[k], local_sem.at[2]).start()

    def loaded(ref, index):
        pltpu.make_async_copy(ref, ref, local_sem.at[index]).wait()

    barrier = pltpu.get_barrier_semaphore()
    partners = [(CORES * z + other, x)]
    partners += [(zrow(o), x) for o in (1, -1)]
    partners += [(r, xcol(o)) for o in (1, -1, 2, -2)]
    for row, col in partners:
        pl.semaphore_signal(barrier, inc=1, device_id={"row": row, "col": col}, device_id_type=MESH)
    pl.semaphore_wait(barrier, len(partners))

    def pass_word(i, hops):
        for o in (hops, -hops):
            pl.semaphore_signal(
                word_sem.at[i], inc=1, device_id={"row": zrow(o), "col": x}, device_id_type=MESH)

    def hello_1():
        pl.semaphore_wait(word_sem.at[0], 2)
        pass_word(1, 1)

    def hello_2():
        pl.semaphore_wait(word_sem.at[1], 2)
        pass_word(2, 2)

    def hello_3():
        pl.semaphore_wait(word_sem.at[2], 2)

    pass_word(0, 1)

    def steps_of(k):
        s = -1 if k % 2 else 1
        zz_row = lambda o: zrow(s * o)
        zz = lambda o: zunit(s * o)
        xx = lambda o: xcol(s * o)
        own_cols = pl.ds(pl.multiple_of(c * half, 128), half)
        other_cols = pl.ds(pl.multiple_of(other * half, 128), half)
        peer = CORES * z + other

        def a_send(o, n, to):
            block_at = g_all.at[k, xx(o)]
            send(k, block_at, block_at, "g", "a2" if n == 2 else "a", r, xx(to))

        def a0():
            if k == 0:
                loaded(g_all.at[:, x], 0)
            for n in (2, 1):
                a_send(0, n, n)
                a_send(0, n, -n)

        def a_pass():
            arrived(k, g_all.at[k, pl.ds(0, 2)], "a2")
            a_send(-2, 4, 2)
            a_send(-2, 3, 1)
            a_send(2, 3, -1)

        def m1():
            arrived(k, g_all.at[k, pl.ds(0, 5)], "a")
            if k == 0:
                loaded(e_v, 1)
            g = g_all[k].reshape(NX * h, g_all.shape[3])
            p = jnp.dot(g, e_v[:, other_cols], preferred_element_type=F32)
            psend[k] = p.astype(BF16).reshape(psend.shape[1:])
            send(k, psend.at[k], precv.at[k], "x", "x", peer, x)
            p = jnp.dot(g, e_v[:, own_cols], preferred_element_type=F32)
            acc[k] = p.reshape(acc.shape[1:])

        def m1_sum():
            arrived(k, precv.at[k], "x")
            acc[k] = acc[k] + precv[k].astype(F32)
            slot = 0
            for arrive, to, units in LEVEL_ONE:
                for o in units:
                    b1s[k, slot] = acc[k, zz(o)].astype(BF16)
                    slot += 1
                n = len(units)
                part = pl.ds(slot - n, n)
                send(k, b1s.at[k, part], b1r.at[k, part], "b1", arrive, zz_row(to), x)

        def level_one_sum(o, slots):
            value = acc[k, zz(o)]
            for slot in slots:
                value = value + b1r[k, slot].astype(F32)
            return value

        def meet(lo, n, arrive, sums):
            arrived(k, b1r.at[k, pl.ds(lo, n)], arrive)
            for slot, o, slots in sums:
                b3s[k, slot] = level_one_sum(o, slots).astype(BF16)
                send(k, b3s.at[k, slot], b3r.at[k, slot], "b3", "b3", zz_row(o), x)

        def meet_far():
            meet(0, 7, "far", ((0, -5, (0, 1, 3, 5)), (1, 5, (2, 4, 6))))

        def meet_near():
            meet(7, 4, "near", ((2, -2, (7, 9)), (3, 2, (8, 10))))

        def to_peer(unit):
            at = sc.at[c, k, unit]
            send(k, at, at, "p", "p", peer, x)

        def c_send(unit, n, o):
            at = sc.at[c, k, unit]
            send(k, at, at, "c", "c%d" % n if n in (2, 5) else "c", zz_row(o), x)

        def final():
            arrived(k, b3r.at[k], "b3")
            if k == 0:
                loaded(ev, 2)
            total = acc[k, z]
            for slot in range(4):
                total = total + b3r[k, slot].astype(F32)
            sc[c, k, z] = (total / (ev[k].astype(F32) + DAMPING)).astype(BF16)
            for n in (5, 2):
                c_send(z, n, n)
                c_send(z, n, -n)
            to_peer(z)

        def fan(n, moves):
            arrived(k, sc.at[c, k, pl.ds(0, 2)], "c%d" % n)
            for t in (1, -1):
                for m in moves:
                    if t * (n + m) != -8:
                        c_send(zz(-t * n), n + m, t * m)
            for t in (1, -1):
                to_peer(zz(-t * n))

        def c_near():
            fan(2, (-1, 1))

        def c_far():
            fan(5, (3, 2, -1, 1))

        def c_end():
            arrived(k, sc.at[c, k, pl.ds(0, 11)], "c")
            for n in (1, 3, 4, 6, 7, 8):
                for t in (1, -1):
                    if t * n != -8:
                        to_peer(zz(-t * n))

        def by_columns(lhs, cols):
            return lax.dot_general(
                lhs, e_v[:, cols], (((1,), (1,)), ((), ())), preferred_element_type=F32)

        def m2():
            p = by_columns(sc[c, k].reshape(NZ * unit_rows, half), own_cols)
            arrived(k, sc.at[other, k], "p")
            p = p + by_columns(sc[other, k].reshape(NZ * unit_rows, half), other_cols)
            res[k] = p.reshape(res.shape[1:])
            for slot, o, to in ((0, -4, -2), (1, -3, -1), (2, 3, 1)):
                d1s[k, slot] = res[k, xx(o)].astype(BF16)
                send(k, d1s.at[k, slot], d1r.at[k, slot], "d1", "d1", r, xx(to))
            for slot, o in ((2, -1), (3, 1)):
                d2s[k, slot] = res[k, xx(o)].astype(BF16)
                send(k, d2s.at[k, slot], d2r.at[k, slot], "d2", "d2", r, xx(o))

        def d2():
            arrived(k, d1r.at[k], "d1")
            for slot, o, ones in ((0, -2, (0, 1)), (1, 2, (2,))):
                value = res[k, xx(o)]
                for one in ones:
                    value = value + d1r[k, one].astype(F32)
                d2s[k, slot] = value.astype(BF16)
                send(k, d2s.at[k, slot], d2r.at[k, slot], "d2", "d2", r, xx(o))

        def df():
            arrived(k, d2r.at[k], "d2")
            total = res[k, x]
            for slot in range(4):
                total = total + d2r[k, slot].astype(F32)
            out[pl.ds(k * h, h)] = total.astype(BF16)

        steps = (a0, a_pass, m1, m1_sum, meet_far, meet_near, final, c_near, c_far, c_end, m2, d2, df)
        return {step.__name__: step for step in steps}

    chunks = {k: steps_of(k) for k in range(CHUNKS)}
    chunks[None] = {step.__name__: step for step in (hello_1, hello_2, hello_3)}
    for k, name in ORDER:
        chunks[k][name]()

    for ref, sent in (
        (g_all.at[:, pl.ds(0, NX - 1)], "g"), (psend, "x"), (b1s, "b1"), (b3s, "b3"),
        (sc.at[c, :, pl.ds(0, NZ - 1)], "c"), (sc.at[c], "p"), (d1s, "d1"), (d2s, "d2"),
    ):
        all_sent(ref, sent)


def on_device(grad_slab, eigenbasis, eigenvalues):
    rows, depth = grad_slab.shape
    width = eigenbasis.shape[1]
    half = width // CORES
    h = rows // CHUNKS
    unit_rows = h * NX // NZ
    unit = (unit_rows, half)
    own = (h, depth)
    any_ = pl.BlockSpec(memory_space=pltpu.HBM)
    vmem = lambda lead, last, kind=BF16: pltpu.VMEM((CHUNKS, *lead, *last), kind)
    return pl.pallas_call(
        kernel,
        out_shape=jax.ShapeDtypeStruct((rows, depth), BF16),
        in_specs=[any_] * 3,
        out_specs=pl.BlockSpec(memory_space=pltpu.VMEM),
        scratch_shapes=[
            pltpu.VMEM(eigenbasis.shape, BF16),
            vmem((NX,), own),
            vmem((), unit),
            vmem((NZ,), unit),
            vmem((NZ,), unit),
            vmem((NZ,), unit, F32),
            vmem((11,), unit),
            vmem((11,), unit),
            vmem((4,), unit),
            vmem((4,), unit),
            pltpu.VMEM((CORES, CHUNKS, NZ, *unit), BF16),
            vmem((NX,), own, F32),
            vmem((3,), own),
            vmem((3,), own),
            vmem((4,), own),
            vmem((4,), own),
            pltpu.SemaphoreType.DMA((3,)),
            pltpu.SemaphoreType.DMA((len(SENT),)),
            pltpu.SemaphoreType.DMA((CHUNKS * len(ARRIVE),)),
            pltpu.SemaphoreType.REGULAR((3,)),
        ],
        compiler_params=pltpu.CompilerParams(
            collective_id=0, has_side_effects=True, vmem_limit_bytes=67043328
        ),
    )(grad_slab, eigenbasis, eigenvalues)


def solution(mesh):
    return jax.shard_map(
        on_device,
        mesh=mesh,
        in_specs=(P(("ckpt", "col"), "row"), P(("ckpt", "row"), "col"), P("ckpt", "col")),
        out_specs=P(("ckpt", "col"), "row"),
        check_vma=False,
    )
```

```python
import functools

import jax
import jax.numpy as jnp
from jax import lax
from jax.experimental import pallas as pl
from jax.experimental.pallas import tpu as pltpu
from jax.sharding import PartitionSpec as P

DAMPING = 0.1
MESH = pl.DeviceIdType.MESH
CORES = 2
CHUNKS = 3
NZ = 16
NX = 8
BF16 = jnp.bfloat16
F32 = jnp.float32
SENT = ("g", "x", "b1", "b3", "c", "p", "d1", "d2")
ARRIVE = ("a2", "a", "x", "far", "near", "b3", "c2", "c5", "c", "p", "d1", "d2")
LEVEL_ONE = (
    ("far", -3, (-8,)), ("far", 1, (-4, 6)), ("far", -1, (-6, 4)), ("far", -2, (-7,)), ("far", 2, (7,)),
    ("near", 1, (-1, 3)), ("near", -1, (-3, 1)),
)
ORDER = (
    (0, "a0"), (1, "a0"), (None, "hello_1"), (0, "a_pass"), (None, "hello_2"),
    (2, "a0"), (1, "a_pass"), (0, "m1"), (0, "m1_sum"), (2, "a_pass"),
    (1, "m1"), (1, "m1_sum"), (2, "m1"), (None, "hello_3"), (0, "meet_far"),
    (2, "m1_sum"), (1, "meet_far"), (0, "meet_near"), (1, "meet_near"), (2, "meet_far"),
    (2, "meet_near"), (0, "final"), (1, "final"), (2, "final"), (0, "c_near"),
    (0, "c_far"), (1, "c_near"), (1, "c_far"), (2, "c_near"), (2, "c_far"),
    (0, "c_end"), (0, "m2"), (1, "c_end"), (0, "m2_sum"), (1, "m2"),
    (1, "m2_sum"), (2, "c_end"), (2, "m2"), (2, "m2_sum"), (0, "d2"),
    (1, "d2"), (2, "d2"), (0, "df"), (1, "df"), (2, "df"),
)


def kernel(
    grad, eig, values, out,
    e_v, g_all, ev, psend, precv, acc,
    b1s, b1r, b3s, b3r, sc, res, d1s, d1r, d2s, d2r,
    local_sem, send_sem, recv_sem, word_sem,
):
    r = lax.axis_index("row")
    x = lax.axis_index("col")
    z, c = lax.div(r, CORES), lax.rem(r, CORES)
    other = 1 - c
    unit_rows, half = acc.shape[2], acc.shape[3]
    h = g_all.shape[2]

    def send(k, src, dst, sent, arrive, row, col):
        pltpu.make_async_remote_copy(
            src_ref=src, dst_ref=dst, send_sem=send_sem.at[SENT.index(sent)],
            recv_sem=recv_sem.at[k * len(ARRIVE) + ARRIVE.index(arrive)],
            device_id={"row": row, "col": col}, device_id_type=MESH,
        ).start()

    def pending(ref, sent=0, arrive=0):
        return pltpu.make_async_remote_copy(
            src_ref=ref, dst_ref=ref, send_sem=send_sem.at[sent], recv_sem=recv_sem.at[arrive],
            device_id={"row": CORES * z + other, "col": x}, device_id_type=MESH,
        )

    def arrived(k, ref, arrive):
        pending(ref, arrive=k * len(ARRIVE) + ARRIVE.index(arrive)).wait_recv()

    def all_sent(ref, sent):
        pending(ref, sent=SENT.index(sent)).wait_send()

    def zrow(offset):
        return lax.rem(z + (offset + NZ), NZ) * CORES + c

    def zunit(offset):
        return lax.rem(z + (offset + NZ), NZ)

    def xcol(offset):
        return lax.rem(x + (offset + NX), NX)

    for k in range(CHUNKS):
        pltpu.make_async_copy(grad.at[pl.ds(k * h, h)], g_all.at[k, x], local_sem.at[0]).start()
    pltpu.make_async_copy(eig, e_v, local_sem.at[1]).start()
    block = lax.div(z, 2)
    for k in range(CHUNKS):
        first = block * (CHUNKS * h) + k * h + lax.rem(z, 2) * unit_rows
        pltpu.make_async_copy(
            values.at[pl.ds(pl.multiple_of(first, unit_rows), unit_rows),
                      pl.ds(pl.multiple_of(c * half, 128), half)],
            ev.at[k], local_sem.at[2]).start()

    def loaded(ref, index):
        pltpu.make_async_copy(ref, ref, local_sem.at[index]).wait()

    barrier = pltpu.get_barrier_semaphore()
    partners = [(CORES * z + other, x)]
    partners += [(zrow(o), x) for o in (1, -1)]
    partners += [(r, xcol(o)) for o in (1, -1, 2, -2)]
    for row, col in partners:
        pl.semaphore_signal(barrier, inc=1, device_id={"row": row, "col": col}, device_id_type=MESH)
    pl.semaphore_wait(barrier, len(partners))

    def pass_word(i, hops):
        for o in (hops, -hops):
            pl.semaphore_signal(
                word_sem.at[i], inc=1, device_id={"row": zrow(o), "col": x}, device_id_type=MESH)

    def hello_1():
        pl.semaphore_wait(word_sem.at[0], 2)
        pass_word(1, 1)

    def hello_2():
        pl.semaphore_wait(word_sem.at[1], 2)
        pass_word(2, 2)

    def hello_3():
        pl.semaphore_wait(word_sem.at[2], 2)

    pass_word(0, 1)

    def steps_of(k):
        s = -1 if k % 2 else 1
        zz_row = lambda o: zrow(s * o)
        zz = lambda o: zunit(s * o)
        xx = lambda o: xcol(s * o)
        own_cols = pl.ds(pl.multiple_of(c * half, 128), half)
        other_cols = pl.ds(pl.multiple_of(other * half, 128), half)
        peer = CORES * z + other

        def a_send(o, n, to):
            block_at = g_all.at[k, xx(o)]
            send(k, block_at, block_at, "g", "a2" if n == 2 else "a", r, xx(to))

        def a0():
            if k == 0:
                loaded(g_all.at[:, x], 0)
            for n in (2, 1):
                a_send(0, n, n)
                a_send(0, n, -n)

        def a_pass():
            arrived(k, g_all.at[k, pl.ds(0, 2)], "a2")
            a_send(-2, 4, 2)
            a_send(-2, 3, 1)
            a_send(2, 3, -1)

        def m1():
            arrived(k, g_all.at[k, pl.ds(0, 5)], "a")
            if k == 0:
                loaded(e_v, 1)
            g = g_all[k].reshape(NX * h, g_all.shape[3])
            p = jnp.dot(g, e_v[:, other_cols], preferred_element_type=F32)
            psend[k] = p.astype(BF16).reshape(psend.shape[1:])
            send(k, psend.at[k], precv.at[k], "x", "x", peer, x)
            p = jnp.dot(g, e_v[:, own_cols], preferred_element_type=F32)
            acc[k] = p.reshape(acc.shape[1:])

        def m1_sum():
            arrived(k, precv.at[k], "x")
            acc[k] = acc[k] + precv[k].astype(F32)
            slot = 0
            for arrive, to, units in LEVEL_ONE:
                for o in units:
                    b1s[k, slot] = acc[k, zz(o)].astype(BF16)
                    slot += 1
                n = len(units)
                part = pl.ds(slot - n, n)
                send(k, b1s.at[k, part], b1r.at[k, part], "b1", arrive, zz_row(to), x)

        def level_one_sum(o, slots):
            value = acc[k, zz(o)]
            for slot in slots:
                value = value + b1r[k, slot].astype(F32)
            return value

        def meet(lo, n, arrive, sums):
            arrived(k, b1r.at[k, pl.ds(lo, n)], arrive)
            for slot, o, slots in sums:
                b3s[k, slot] = level_one_sum(o, slots).astype(BF16)
                send(k, b3s.at[k, slot], b3r.at[k, slot], "b3", "b3", zz_row(o), x)

        def meet_far():
            meet(0, 7, "far", ((0, -5, (0, 1, 3, 5)), (1, 5, (2, 4, 6))))

        def meet_near():
            meet(7, 4, "near", ((2, -2, (7, 9)), (3, 2, (8, 10))))

        def to_peer(unit):
            at = sc.at[c, k, unit]
            send(k, at, at, "p", "p", peer, x)

        def c_send(unit, n, o):
            at = sc.at[c, k, unit]
            send(k, at, at, "c", "c%d" % n if n in (2, 5) else "c", zz_row(o), x)

        def final():
            arrived(k, b3r.at[k], "b3")
            if k == 0:
                loaded(ev, 2)
            total = acc[k, z]
            for slot in range(4):
                total = total + b3r[k, slot].astype(F32)
            sc[c, k, z] = (total / (ev[k].astype(F32) + DAMPING)).astype(BF16)
            for n in (5, 2):
                c_send(z, n, n)
                c_send(z, n, -n)
            to_peer(z)

        def fan(n, moves):
            arrived(k, sc.at[c, k, pl.ds(0, 2)], "c%d" % n)
            for t in (1, -1):
                for m in moves:
                    if t * (n + m) != -8:
                        c_send(zz(-t * n), n + m, t * m)
            for t in (1, -1):
                to_peer(zz(-t * n))

        def c_near():
            fan(2, (-1, 1))

        def c_far():
            fan(5, (3, 2, -1, 1))

        def c_end():
            arrived(k, sc.at[c, k, pl.ds(0, 11)], "c")
            for n in (1, 3, 4, 6, 7, 8):
                for t in (1, -1):
                    if t * n != -8:
                        to_peer(zz(-t * n))

        def by_columns(lhs, cols):
            return lax.dot_general(
                lhs, e_v[:, cols], (((1,), (1,)), ((), ())), preferred_element_type=F32)

        def m2():
            p = by_columns(sc[c, k].reshape(NZ * unit_rows, half), own_cols)
            res[k] = p.reshape(res.shape[1:])

        def m2_sum():
            arrived(k, sc.at[other, k], "p")
            p = by_columns(sc[other, k].reshape(NZ * unit_rows, half), other_cols)
            res[k] = res[k] + p.reshape(res.shape[1:])
            for slot, o, to in ((0, -4, -2), (1, -3, -1), (2, 3, 1)):
                d1s[k, slot] = res[k, xx(o)].astype(BF16)
                send(k, d1s.at[k, slot], d1r.at[k, slot], "d1", "d1", r, xx(to))
            for slot, o in ((2, -1), (3, 1)):
                d2s[k, slot] = res[k, xx(o)].astype(BF16)
                send(k, d2s.at[k, slot], d2r.at[k, slot], "d2", "d2", r, xx(o))

        def d2():
            arrived(k, d1r.at[k], "d1")
            for slot, o, ones in ((0, -2, (0, 1)), (1, 2, (2,))):
                value = res[k, xx(o)]
                for one in ones:
                    value = value + d1r[k, one].astype(F32)
                d2s[k, slot] = value.astype(BF16)
                send(k, d2s.at[k, slot], d2r.at[k, slot], "d2", "d2", r, xx(o))

        def df():
            arrived(k, d2r.at[k], "d2")
            total = res[k, x]
            for slot in range(4):
                total = total + d2r[k, slot].astype(F32)
            out[pl.ds(k * h, h)] = total.astype(BF16)

        steps = (a0, a_pass, m1, m1_sum, meet_far, meet_near, final, c_near, c_far, c_end, m2, m2_sum, d2, df)
        return {step.__name__: step for step in steps}

    chunks = {k: steps_of(k) for k in range(CHUNKS)}
    chunks[None] = {step.__name__: step for step in (hello_1, hello_2, hello_3)}
    for k, name in ORDER:
        chunks[k][name]()

    for ref, sent in (
        (g_all.at[:, pl.ds(0, NX - 1)], "g"), (psend, "x"), (b1s, "b1"), (b3s, "b3"),
        (sc.at[c, :, pl.ds(0, NZ - 1)], "c"), (sc.at[c], "p"), (d1s, "d1"), (d2s, "d2"),
    ):
        all_sent(ref, sent)


def on_device(grad_slab, eigenbasis, eigenvalues):
    rows, depth = grad_slab.shape
    width = eigenbasis.shape[1]
    half = width // CORES
    h = rows // CHUNKS
    unit_rows = h * NX // NZ
    unit = (unit_rows, half)
    own = (h, depth)
    any_ = pl.BlockSpec(memory_space=pltpu.HBM)
    vmem = lambda lead, last, kind=BF16: pltpu.VMEM((CHUNKS, *lead, *last), kind)
    return pl.pallas_call(
        kernel,
        out_shape=jax.ShapeDtypeStruct((rows, depth), BF16),
        in_specs=[any_] * 3,
        out_specs=pl.BlockSpec(memory_space=pltpu.VMEM),
        scratch_shapes=[
            pltpu.VMEM(eigenbasis.shape, BF16),
            vmem((NX,), own),
            vmem((), unit),
            vmem((NZ,), unit),
            vmem((NZ,), unit),
            vmem((NZ,), unit, F32),
            vmem((11,), unit),
            vmem((11,), unit),
            vmem((4,), unit),
            vmem((4,), unit),
            pltpu.VMEM((CORES, CHUNKS, NZ, *unit), BF16),
            vmem((NX,), own, F32),
            vmem((3,), own),
            vmem((3,), own),
            vmem((4,), own),
            vmem((4,), own),
            pltpu.SemaphoreType.DMA((3,)),
            pltpu.SemaphoreType.DMA((len(SENT),)),
            pltpu.SemaphoreType.DMA((CHUNKS * len(ARRIVE),)),
            pltpu.SemaphoreType.REGULAR((3,)),
        ],
        compiler_params=pltpu.CompilerParams(
            collective_id=0, has_side_effects=True, vmem_limit_bytes=67043328
        ),
    )(grad_slab, eigenbasis, eigenvalues)


def solution(mesh):
    return jax.shard_map(
        on_device,
        mesh=mesh,
        in_specs=(P(("ckpt", "col"), "row"), P(("ckpt", "row"), "col"), P("ckpt", "col")),
        out_specs=P(("ckpt", "col"), "row"),
        check_vma=False,
    )
```
